32 devices in a mesh: row: 16 (over z, x, core), col: 2 (over y).
Axes of the slice: x: 2, y: 2, z: 4, core: 2. Of those that a mesh axis runs over, the one named last changes fastest.
Arguments:
- density: float32 [128, 16, 128, 128], P('row', 'col'), may hold values from -0.75 to 0.75
- columns: int32 [128, 16], P('row', 'col'), may hold values from -1 to 127, as said below
Outputs:
- purified: float32 [128, 16, 128, 128], P('row', 'col')
The draws below stay inside these ranges and needn't reach their ends.
Inputs may be any that keep to these rules, and one draw needn't show every extreme that they name: Block row i lists its occupied block columns in its first slots and -1 in the rest; it has 2 to 16 occupied slots, slot 0 holds column i, the listed columns of a row are distinct, and each listed column j satisfies (j - i) mod 128 <= 8 or (j - i) mod 128 >= 120.
All inputs are finite; a program needn't handle non-finite values.
Results may differ from the reference program's by a relative error of at most 0.0003.
Values sent between devices are 32-bit elements; how exact they have to be, the bound alone decides.
A program may use at most 128 MiB of HBM per device.

```python
import jax
import jax.numpy as jnp
from jax import lax

B = 128
S = 16
W = 8
NB = 128


def draw_columns(key, part):
    count_key, order_key = jax.random.split(jax.random.fold_in(key, 11))
    counts = jax.random.randint(count_key, (NB,), 2, S + 1).astype(jnp.int32)
    counts = counts.at[0].set(S)
    offsets = jnp.concatenate([jnp.arange(-W, 0), jnp.arange(1, W + 1)]).astype(jnp.int32)
    row_keys = jax.random.split(order_key, NB)
    shuffled = jax.vmap(lambda single: jax.random.permutation(single, offsets))(row_keys)
    chosen = jnp.concatenate([jnp.zeros((NB, 1), jnp.int32), shuffled[:, :S - 1]], axis=1)
    rows = jnp.arange(NB, dtype=jnp.int32)[:, None]
    listed = (rows + chosen) % NB
    slot_ids = jnp.arange(S, dtype=jnp.int32)[None, :]
    return jnp.where(slot_ids < counts[:, None], listed, -1).astype(jnp.int32)


def level_of(key, extent, cuts, smallest, top_value):
    level = 1.0
    for axis_at, parts in cuts:
        heights = jax.random.uniform(jax.random.fold_in(jax.random.fold_in(key, 6), axis_at), (parts,), jnp.float32, smallest / len(cuts), top_value / len(cuts))
        level = level * jnp.repeat(jnp.exp(heights), extent[axis_at] // parts).reshape((-1,) + (1,) * (len(extent) - 1 - axis_at))
    return level


def noise(stream_key, extent, scale, limit, shards=(), kind=jnp.bfloat16):
    loudness = level_of(stream_key, extent, shards, -0.22, 0.18) if shards else 1.0
    entries = jax.random.normal(stream_key, extent, jnp.float32) * scale * loudness
    return jnp.minimum(jnp.maximum(entries, -limit), limit).astype(kind)


def setup_inputs(seed: int = 0) -> dict:
    key_list = jax.random.split(jax.random.key(seed), 3)
    density = noise(key_list[0], (NB, S, B, B), 0.125, 0.75, ((0, 16), (1, 2)), jnp.float32)
    columns = draw_columns(jax.random.fold_in(key_list[2], 71), 0)
    return dict(density=density, columns=columns)


def pattern_product(left, right, columns):
    slots = columns.shape[1]

    def one_row(index):
        own = columns[index]
        safe = jnp.where(own >= 0, own, 0)
        candidate = columns[safe]
        matched = (candidate[None, :, :] == own[:, None, None]) & (own >= 0)[:, None, None] & (own >= 0)[None, :, None]
        weights = matched.astype(jnp.float32)
        chosen = jnp.einsum("sab,abxy->saxy", weights, right[safe], precision=lax.Precision.HIGHEST)
        return jnp.einsum("axk,sakc->sxc", left[index], chosen, precision=lax.Precision.HIGHEST)

    return lax.map(one_row, jnp.arange(columns.shape[0], dtype=jnp.int32))


def reference(density, columns):
    square = pattern_product(density, density, columns)
    cube = pattern_product(square, density, columns)
    return 3.0 * square - 2.0 * cube
```

```python
import functools

import jax
import jax.numpy as jnp
from jax import lax
from jax.experimental import pallas as pl
from jax.experimental.pallas import tpu as pltpu
from jax.sharding import PartitionSpec as P

W = 8
GROUP = 4
UNROLL = 2


def shifted(value, step):
    count = lax.axis_size("row")
    return lax.ppermute(value, "row", [(i, (i + step) % count) for i in range(count)])


def work_lists(ext_columns, own_start, panel_start, row_start, block_count, rows):
    slots = ext_columns.shape[1]
    own = lax.dynamic_slice_in_dim(ext_columns, W + own_start, rows)
    row_ids = jnp.arange(rows, dtype=jnp.int32)[:, None]
    offset = (own - (row_start + own_start + row_ids) + W) % block_count - W
    ext_row = jnp.where(own >= 0, W + own_start + row_ids + offset, 0)
    candidate = ext_columns[ext_row]
    matched = (
        (candidate[:, None] == own[:, :, None, None])
        & (own >= 0)[:, :, None, None]
        & (own >= 0)[:, None, :, None]
    )
    present = jnp.any(matched, axis=-1)
    slot_ids = jnp.arange(slots, dtype=jnp.int32)
    picked = jnp.sum(jnp.where(matched, slot_ids, 0), axis=-1)
    right = jnp.where(present, (ext_row - panel_start)[:, None, :] * slots + picked, 0)
    left = jnp.broadcast_to((row_ids * slots + slot_ids)[:, None, :], present.shape)
    targets = rows * slots
    present = present.reshape(targets, slots)
    rank = jnp.cumsum(present.astype(jnp.int32), axis=-1) - 1
    counts = jnp.sum(present.astype(jnp.int32), axis=-1)
    chosen = present[:, :, None] & (rank[:, :, None] == slot_ids)
    filled = slot_ids < counts[:, None]
    left_list = jnp.sum(jnp.where(chosen, left.reshape(targets, slots)[:, :, None], 0), axis=1)
    left_list = jnp.where(filled, left_list, targets)
    right_list = jnp.sum(jnp.where(chosen, right.reshape(targets, slots)[:, :, None], 0), axis=1)
    per_target = slots // GROUP
    chunks = (counts + GROUP - 1) // GROUP
    ends = jnp.cumsum(chunks)
    total = ends[-1]
    turns = jnp.arange(targets * per_target, dtype=jnp.int32)
    target = jnp.minimum(
        jnp.sum((ends[None, :] <= turns[:, None]).astype(jnp.int32), axis=1), targets - 1
    )
    place = jnp.clip(turns - (ends - chunks)[target], 0, per_target - 1)
    at = target * per_target + place
    live = (turns < total)[:, None]
    left_chunks = jnp.where(live, left_list.reshape(-1, GROUP)[at], targets)
    right_chunks = jnp.where(live, right_list.reshape(-1, GROUP)[at], 0)
    return total, target, left_chunks.reshape(-1), right_chunks.reshape(-1)


def split(value):
    high = value.astype(jnp.bfloat16)
    low = (value - high.astype(jnp.float32)).astype(jnp.bfloat16)
    return high, low


def kernel(sizes, slots, targets, meta, target_list, left_list, right_list, *refs):
    pieces = refs[: len(sizes)]
    out, stage, panel, left, square, sems = refs[len(sizes) :]
    order = out.shape[-1]
    starts = []
    at = 0
    for rows, width in sizes:
        starts.append(at)
        at += rows * width
    copies = [
        pltpu.make_async_copy(
            piece, stage.at[pl.ds(start, rows * width)], sems.at[number]
        )
        for number, (piece, start, (rows, width)) in enumerate(zip(pieces, starts, sizes))
    ]
    for copy in copies:
        copy.start()
    left[targets] = jnp.zeros((2 * order, order), jnp.bfloat16)

    def clear(block, carry):
        square[block] = jnp.zeros((order, order), jnp.float32)
        return carry

    lax.fori_loop(0, targets, clear, 0)
    for number, (copy, start, (rows, width)) in enumerate(zip(copies, starts, sizes)):
        copy.wait()
        first = meta[2 + number]

        def place(block, carry, start=start, width=width, first=first):
            high, low = split(stage[start + block])
            where = first + (block // width) * slots + block % width
            panel[where, :, :order] = high
            panel[where, :, order:] = low
            return carry

        lax.fori_loop(0, rows * width, place, 0)
    left_base = meta[1]

    def load_left(block, carry):
        left[block, :order] = panel[left_base + block, :, :order]
        left[block, order:] = panel[left_base + block, :, order:]
        return carry

    lax.fori_loop(0, targets, load_left, 0)
    rounds = (meta[0] + UNROLL - 1) // UNROLL

    def product(result, factor):
        def step(turn, carry):
            sums = []
            for inner in range(UNROLL):
                begin = (turn * UNROLL + inner) * GROUP
                lhs = jnp.concatenate([left[left_list[begin + g]] for g in range(GROUP)], axis=1)
                rhs = jnp.concatenate([panel[right_list[begin + g]] for g in range(GROUP)], axis=0)
                both = jnp.dot(lhs, rhs, preferred_element_type=jnp.float32)
                sums.append(
                    both[:order, :order]
                    + (both[:order, order:] + both[order:, :order])
                    + both[order:, order:]
                )
            for inner in range(UNROLL):
                target = target_list[turn * UNROLL + inner]
                result[target] += sums[inner] if factor == 1.0 else factor * sums[inner]
            return carry

        lax.fori_loop(0, rounds, step, 0)

    product(square, 1.0)

    def middle(block, carry):
        value = square[block]
        high, low = split(value)
        left[block, :order] = high
        left[block, order:] = low
        out[block] = 3.0 * value
        return carry

    lax.fori_loop(0, targets, middle, 0)
    product(out, -2.0)


def products(total, left_base, firsts, lists, pieces, panel_rows, slots, rows):
    order = pieces[0].shape[-1]
    sizes = tuple((piece.shape[0], piece.shape[1]) for piece in pieces)
    targets = rows * slots
    meta = jnp.stack([jnp.asarray(v, jnp.int32) for v in (total, left_base, *firsts)])
    blocks = sum(a * b for a, b in sizes)
    any_spec = pl.BlockSpec(memory_space=pl.ANY)
    smem_spec = pl.BlockSpec(memory_space=pltpu.SMEM)
    return pl.pallas_call(
        functools.partial(kernel, sizes, slots, targets),
        out_shape=jax.ShapeDtypeStruct((targets, order, order), jnp.float32),
        in_specs=[smem_spec] * 4 + [any_spec] * len(pieces),
        out_specs=pl.BlockSpec(memory_space=pltpu.VMEM),
        scratch_shapes=[
            pltpu.VMEM((blocks, order, order), jnp.float32),
            pltpu.VMEM((panel_rows * slots, order, 2 * order), jnp.bfloat16),
            pltpu.VMEM((targets + 1, 2 * order, order), jnp.bfloat16),
            pltpu.VMEM((targets, order, order), jnp.float32),
            pltpu.SemaphoreType.DMA((len(pieces),)),
        ],
        compiler_params=pltpu.CompilerParams(vmem_limit_bytes=62 * 1024 * 1024),
        cost_estimate=pl.CostEstimate(
            flops=8 * targets * 8 * order**3,
            bytes_accessed=blocks * order * order * 4,
            transcendentals=0,
        ),
    )(meta, *lists, *[piece.reshape(-1, order, order) for piece in pieces])


def per_device(density, columns):
    local_rows, local_slots, order, _ = density.shape
    row_count = lax.axis_size("row")
    column_count = lax.axis_size("col")
    slots = local_slots * column_count
    rows = local_rows // column_count
    block_count = local_rows * row_count
    row_start = lax.axis_index("row") * local_rows
    column = lax.axis_index("col")
    own_start = column * rows
    full_columns = lax.all_gather(columns, "col", axis=1, tiled=True)
    ext_columns = jnp.concatenate(
        [
            shifted(full_columns[local_rows - W :], 1),
            full_columns,
            shifted(full_columns[:W], -1),
        ]
    )
    trimmed = column_count == 2 and local_rows == W
    panel_start = own_start if trimmed else 0
    total, *lists = work_lists(
        ext_columns, own_start, panel_start, row_start, block_count, rows
    )
    if trimmed:
        ring = [(2 * i, 2 * ((i + 1) % row_count)) for i in range(row_count)]
        back = [(2 * ((i + 1) % row_count) + 1, 2 * i + 1) for i in range(row_count)]
        far_pairs = ring + back
        near_pairs = [(b, a) for a, b in far_pairs]
        peers = [(i, i ^ 1) for i in range(2 * row_count)]
        axes = ("row", "col")
        own_near = lax.dynamic_slice_in_dim(density, column * rows, rows)
        other = lax.ppermute(density, axes, peers)
        far_own = lax.ppermute(density, axes, far_pairs)
        near_own = lax.ppermute(own_near, axes, near_pairs)
        other_near = lax.dynamic_slice_in_dim(other, column * rows, rows)
        far_other = lax.ppermute(other, axes, far_pairs)
        near_other = lax.ppermute(other_near, axes, near_pairs)
        pieces = [density, far_own, near_own, other, far_other, near_other]
        own_row = W - own_start
        far_row = jnp.where(column == 0, 0, rows + local_rows)
        near_row = jnp.where(column == 0, W + local_rows, 0)
        here = column * local_slots
        there = (1 - column) * local_slots
        firsts = [
            own_row * slots + here,
            far_row * slots + here,
            near_row * slots + here,
            own_row * slots + there,
            far_row * slots + there,
            near_row * slots + there,
        ]
        panel_rows = 2 * W + rows
    else:
        full_rows = lax.all_gather(density, "col", axis=1, tiled=True)
        pieces = [
            shifted(full_rows[local_rows - W :], 1),
            full_rows,
            shifted(full_rows[:W], -1),
        ]
        firsts = [0, W * slots, (W + local_rows) * slots]
        panel_rows = 2 * W + local_rows
    left_base = (W + own_start - panel_start) * slots
    result = products(total, left_base, firsts, lists, pieces, panel_rows, slots, rows)
    result = result.reshape(rows, slots, order, order)
    if column_count != 2:
        return lax.all_to_all(result, "col", split_axis=1, concat_axis=0, tiled=True)
    kept = lax.dynamic_slice_in_dim(result, column * local_slots, local_slots, axis=1)
    sent = lax.dynamic_slice_in_dim(result, (1 - column) * local_slots, local_slots, axis=1)
    arrived = lax.ppermute(sent, "col", [(0, 1), (1, 0)])
    return jnp.where(
        column == 0,
        jnp.concatenate([kept, arrived]),
        jnp.concatenate([arrived, kept]),
    )


def solution(mesh):
    in_specs = (P("row", "col", None, None), P("row", "col"))
    out_specs = P("row", "col", None, None)
    return jax.shard_map(
        per_device, mesh=mesh, in_specs=in_specs, out_specs=out_specs, check_vma=False
    )
```

```python
import functools

import jax
import jax.numpy as jnp
from jax import lax
from jax.experimental import pallas as pl
from jax.experimental.pallas import tpu as pltpu
from jax.sharding import PartitionSpec as P

W = 8
GROUP = 4
UNROLL = 2


def shifted(value, step):
    count = lax.axis_size("row")
    return lax.ppermute(value, "row", [(i, (i + step) % count) for i in range(count)])


def work_lists(ext_columns, own_start, panel_start, row_start, block_count, rows):
    slots = ext_columns.shape[1]
    own = lax.dynamic_slice_in_dim(ext_columns, W + own_start, rows)
    row_ids = jnp.arange(rows, dtype=jnp.int32)[:, None]
    offset = (own - (row_start + own_start + row_ids) + W) % block_count - W
    ext_row = jnp.where(own >= 0, W + own_start + row_ids + offset, 0)
    candidate = ext_columns[ext_row]
    matched = (
        (candidate[:, None] == own[:, :, None, None])
        & (own >= 0)[:, :, None, None]
        & (own >= 0)[:, None, :, None]
    )
    present = jnp.any(matched, axis=-1)
    slot_ids = jnp.arange(slots, dtype=jnp.int32)
    picked = jnp.sum(jnp.where(matched, slot_ids, 0), axis=-1)
    right = jnp.where(present, (ext_row - panel_start)[:, None, :] * slots + picked, 0)
    left = jnp.broadcast_to((row_ids * slots + slot_ids)[:, None, :], present.shape)
    targets = rows * slots
    present = present.reshape(targets, slots)
    rank = jnp.cumsum(present.astype(jnp.int32), axis=-1) - 1
    counts = jnp.sum(present.astype(jnp.int32), axis=-1)
    chosen = present[:, :, None] & (rank[:, :, None] == slot_ids)
    filled = slot_ids < counts[:, None]
    left_list = jnp.sum(jnp.where(chosen, left.reshape(targets, slots)[:, :, None], 0), axis=1)
    left_list = jnp.where(filled, left_list, targets)
    right_list = jnp.sum(jnp.where(chosen, right.reshape(targets, slots)[:, :, None], 0), axis=1)
    per_target = slots // GROUP
    chunks = (counts + GROUP - 1) // GROUP
    ends = jnp.cumsum(chunks)
    total = ends[-1]
    turns = jnp.arange(targets * per_target, dtype=jnp.int32)
    target = jnp.minimum(
        jnp.sum((ends[None, :] <= turns[:, None]).astype(jnp.int32), axis=1), targets - 1
    )
    place = jnp.clip(turns - (ends - chunks)[target], 0, per_target - 1)
    at = target * per_target + place
    live = (turns < total)[:, None]
    left_chunks = jnp.where(live, left_list.reshape(-1, GROUP)[at], targets)
    right_chunks = jnp.where(live, right_list.reshape(-1, GROUP)[at], 0)
    return total, target, left_chunks.reshape(-1), right_chunks.reshape(-1)


def split(value):
    high = value.astype(jnp.bfloat16)
    low = (value - high.astype(jnp.float32)).astype(jnp.bfloat16)
    return high, low


def kernel(sizes, slots, targets, meta, target_list, left_list, right_list, *refs):
    pieces = refs[: len(sizes)]
    out, stage, panel, left, square, sems = refs[len(sizes) :]
    order = out.shape[-1]
    starts = []
    at = 0
    for rows, width in sizes:
        starts.append(at)
        at += rows * width
    copies = [
        pltpu.make_async_copy(
            piece, stage.at[pl.ds(start, rows * width)], sems.at[number]
        )
        for number, (piece, start, (rows, width)) in enumerate(zip(pieces, starts, sizes))
    ]
    for copy in copies:
        copy.start()
    left[targets] = jnp.zeros((2 * order, order), jnp.bfloat16)

    def clear(block, carry):
        square[block] = jnp.zeros((order, order), jnp.float32)
        return carry

    lax.fori_loop(0, targets, clear, 0)
    for number, (copy, start, (rows, width)) in enumerate(zip(copies, starts, sizes)):
        copy.wait()
        first = meta[2 + number]

        def place(block, carry, start=start, width=width, first=first):
            high, low = split(stage[start + block])
            where = first + (block // width) * slots + block % width
            panel[where, :, :order] = high
            panel[where, :, order:] = low
            return carry

        lax.fori_loop(0, rows * width, place, 0)
    left_base = meta[1]

    def load_left(block, carry):
        left[block, :order] = panel[left_base + block, :, :order]
        left[block, order:] = panel[left_base + block, :, order:]
        return carry

    lax.fori_loop(0, targets, load_left, 0)
    rounds = (meta[0] + UNROLL - 1) // UNROLL

    def product(result, factor):
        def step(turn, carry):
            sums = []
            for inner in range(UNROLL):
                begin = (turn * UNROLL + inner) * GROUP
                lhs = jnp.concatenate([left[left_list[begin + g]] for g in range(GROUP)], axis=1)
                rhs = jnp.concatenate([panel[right_list[begin + g]] for g in range(GROUP)], axis=0)
                both = jnp.dot(lhs, rhs, preferred_element_type=jnp.float32)
                sums.append(
                    both[:order, :order]
                    + (both[:order, order:] + both[order:, :order])
                    + both[order:, order:]
                )
            for inner in range(UNROLL):
                target = target_list[turn * UNROLL + inner]
                result[target] += sums[inner] if factor == 1.0 else factor * sums[inner]
            return carry

        lax.fori_loop(0, rounds, step, 0)

    product(square, 1.0)

    def middle(block, carry):
        value = square[block]
        high, low = split(value)
        left[block, :order] = high
        left[block, order:] = low
        out[block] = 3.0 * value
        return carry

    lax.fori_loop(0, targets, middle, 0)
    product(out, -2.0)


def products(total, left_base, firsts, lists, pieces, panel_rows, slots, rows):
    order = pieces[0].shape[-1]
    sizes = tuple((piece.shape[0], piece.shape[1]) for piece in pieces)
    targets = rows * slots
    meta = jnp.stack([jnp.asarray(v, jnp.int32) for v in (total, left_base, *firsts)])
    blocks = sum(a * b for a, b in sizes)
    any_spec = pl.BlockSpec(memory_space=pl.ANY)
    smem_spec = pl.BlockSpec(memory_space=pltpu.SMEM)
    return pl.pallas_call(
        functools.partial(kernel, sizes, slots, targets),
        out_shape=jax.ShapeDtypeStruct((targets, order, order), jnp.float32),
        in_specs=[smem_spec] * 4 + [any_spec] * len(pieces),
        out_specs=pl.BlockSpec(memory_space=pltpu.VMEM),
        scratch_shapes=[
            pltpu.VMEM((blocks, order, order), jnp.float32),
            pltpu.VMEM((panel_rows * slots, order, 2 * order), jnp.bfloat16),
            pltpu.VMEM((targets + 1, 2 * order, order), jnp.bfloat16),
            pltpu.VMEM((targets, order, order), jnp.float32),
            pltpu.SemaphoreType.DMA((len(pieces),)),
        ],
        compiler_params=pltpu.CompilerParams(vmem_limit_bytes=62 * 1024 * 1024),
        cost_estimate=pl.CostEstimate(
            flops=8 * targets * 8 * order**3,
            bytes_accessed=blocks * order * order * 4,
            transcendentals=0,
        ),
    )(meta, *lists, *[piece.reshape(-1, order, order) for piece in pieces])


def per_device(density, columns):
    local_rows, local_slots, order, _ = density.shape
    row_count = lax.axis_size("row")
    column_count = lax.axis_size("col")
    slots = local_slots * column_count
    rows = local_rows // column_count
    block_count = local_rows * row_count
    row_start = lax.axis_index("row") * local_rows
    column = lax.axis_index("col")
    own_start = column * rows
    gathered = lax.all_gather(columns, ("row", "col"))
    density, gathered = lax.optimization_barrier((density, gathered))
    gathered = gathered.reshape(row_count, column_count, local_rows, local_slots)
    all_columns = gathered.transpose(0, 2, 1, 3).reshape(block_count, slots)
    wrapped = jnp.concatenate([all_columns[-W:], all_columns, all_columns[:W]])
    ext_columns = lax.dynamic_slice_in_dim(wrapped, row_start, local_rows + 2 * W)
    trimmed = column_count == 2 and local_rows == W
    panel_start = own_start if trimmed else 0
    total, *lists = work_lists(
        ext_columns, own_start, panel_start, row_start, block_count, rows
    )
    if trimmed:
        ring = [(2 * i, 2 * ((i + 1) % row_count)) for i in range(row_count)]
        back = [(2 * ((i + 1) % row_count) + 1, 2 * i + 1) for i in range(row_count)]
        far_pairs = ring + back
        near_pairs = [(b, a) for a, b in far_pairs]
        peers = [(i, i ^ 1) for i in range(2 * row_count)]
        axes = ("row", "col")
        near_at = column * rows
        rest_at = (1 - column) * rows
        own_near = lax.dynamic_slice_in_dim(density, near_at, rows)
        own_rest = lax.dynamic_slice_in_dim(density, rest_at, rows)
        other_near = lax.ppermute(own_rest, axes, peers)
        far_own = lax.ppermute(density, axes, far_pairs)
        near_own = lax.ppermute(own_near, axes, near_pairs)
        other_rest = lax.ppermute(own_near, axes, peers)
        near_other = lax.ppermute(other_near, axes, near_pairs)
        far_other_near = lax.ppermute(other_near, axes, far_pairs)
        far_other_rest = lax.ppermute(other_rest, axes, far_pairs)
        pieces = [
            density,
            far_own,
            near_own,
            other_near,
            other_rest,
            near_other,
            far_other_near,
            far_other_rest,
        ]
        own_row = W - own_start
        far_row = jnp.where(column == 0, 0, rows + local_rows)
        near_row = jnp.where(column == 0, W + local_rows, 0)
        here = column * local_slots
        there = (1 - column) * local_slots
        firsts = [
            own_row * slots + here,
            far_row * slots + here,
            near_row * slots + here,
            (own_row + near_at) * slots + there,
            (own_row + rest_at) * slots + there,
            near_row * slots + there,
            (far_row + near_at) * slots + there,
            (far_row + rest_at) * slots + there,
        ]
        panel_rows = 2 * W + rows
    else:
        full_rows = lax.all_gather(density, "col", axis=1, tiled=True)
        pieces = [
            shifted(full_rows[local_rows - W :], 1),
            full_rows,
            shifted(full_rows[:W], -1),
        ]
        firsts = [0, W * slots, (W + local_rows) * slots]
        panel_rows = 2 * W + local_rows
    left_base = (W + own_start - panel_start) * slots
    result = products(total, left_base, firsts, lists, pieces, panel_rows, slots, rows)
    result = result.reshape(rows, slots, order, order)
    if column_count != 2:
        return lax.all_to_all(result, "col", split_axis=1, concat_axis=0, tiled=True)
    kept = lax.dynamic_slice_in_dim(result, column * local_slots, local_slots, axis=1)
    sent = lax.dynamic_slice_in_dim(result, (1 - column) * local_slots, local_slots, axis=1)
    arrived = lax.ppermute(sent, "col", [(0, 1), (1, 0)])
    return jnp.where(
        column == 0,
        jnp.concatenate([kept, arrived]),
        jnp.concatenate([arrived, kept]),
    )


def solution(mesh):
    in_specs = (P("row", "col", None, None), P("row", "col"))
    out_specs = P("row", "col", None, None)
    return jax.shard_map(
        per_device, mesh=mesh, in_specs=in_specs, out_specs=out_specs, check_vma=False
    )
```

```python
import functools

import jax
import jax.numpy as jnp
from jax import lax
from jax.experimental import pallas as pl
from jax.experimental.pallas import tpu as pltpu
from jax.sharding import PartitionSpec as P

W = 8
GROUP = 4
UNROLL = 2


def shifted(value, step):
    count = lax.axis_size("row")
    return lax.ppermute(value, "row", [(i, (i + step) % count) for i in range(count)])


def work_lists(ext_columns, own_start, panel_start, row_start, block_count, rows):
    slots = ext_columns.shape[1]
    own = lax.dynamic_slice_in_dim(ext_columns, W + own_start, rows)
    row_ids = jnp.arange(rows, dtype=jnp.int32)[:, None]
    offset = (own - (row_start + own_start + row_ids) + W) % block_count - W
    ext_row = jnp.where(own >= 0, W + own_start + row_ids + offset, 0)
    candidate = ext_columns[ext_row]
    matched = (
        (candidate[:, None] == own[:, :, None, None])
        & (own >= 0)[:, :, None, None]
        & (own >= 0)[:, None, :, None]
    )
    present = jnp.any(matched, axis=-1)
    slot_ids = jnp.arange(slots, dtype=jnp.int32)
    picked = jnp.sum(jnp.where(matched, slot_ids, 0), axis=-1)
    right = jnp.where(present, (ext_row - panel_start)[:, None, :] * slots + picked, 0)
    left = jnp.broadcast_to((row_ids * slots + slot_ids)[:, None, :], present.shape)
    targets = rows * slots
    present = present.reshape(targets, slots)
    rank = jnp.cumsum(present.astype(jnp.int32), axis=-1) - 1
    counts = jnp.sum(present.astype(jnp.int32), axis=-1)
    chosen = present[:, :, None] & (rank[:, :, None] == slot_ids)
    filled = slot_ids < counts[:, None]
    left_list = jnp.sum(jnp.where(chosen, left.reshape(targets, slots)[:, :, None], 0), axis=1)
    left_list = jnp.where(filled, left_list, targets)
    right_list = jnp.sum(jnp.where(chosen, right.reshape(targets, slots)[:, :, None], 0), axis=1)
    per_target = slots // GROUP
    chunks = (counts + GROUP - 1) // GROUP
    ends = jnp.cumsum(chunks)
    total = ends[-1]
    turns = jnp.arange(targets * per_target, dtype=jnp.int32)
    target = jnp.minimum(
        jnp.sum((ends[None, :] <= turns[:, None]).astype(jnp.int32), axis=1), targets - 1
    )
    place = jnp.clip(turns - (ends - chunks)[target], 0, per_target - 1)
    at = target * per_target + place
    live = (turns < total)[:, None]
    left_chunks = jnp.where(live, left_list.reshape(-1, GROUP)[at], targets)
    right_chunks = jnp.where(live, right_list.reshape(-1, GROUP)[at], 0)
    return total, target, left_chunks.reshape(-1), right_chunks.reshape(-1)


def split(value):
    high = value.astype(jnp.bfloat16)
    low = (value - high.astype(jnp.float32)).astype(jnp.bfloat16)
    return high, low


def kernel(sizes, slots, targets, meta, target_list, left_list, right_list, *refs):
    pieces = refs[: len(sizes)]
    out, stage, panel, left, square, sems = refs[len(sizes) :]
    order = out.shape[-1]
    starts = []
    at = 0
    for rows, width in sizes:
        starts.append(at)
        at += rows * width
    copies = [
        pltpu.make_async_copy(
            piece, stage.at[pl.ds(start, rows * width)], sems.at[number]
        )
        for number, (piece, start, (rows, width)) in enumerate(zip(pieces, starts, sizes))
    ]
    for copy in copies:
        copy.start()
    left[targets] = jnp.zeros((2 * order, order), jnp.bfloat16)

    def clear(block, carry):
        square[block] = jnp.zeros((order, order), jnp.float32)
        return carry

    lax.fori_loop(0, targets, clear, 0)
    for number, (copy, start, (rows, width)) in enumerate(zip(copies, starts, sizes)):
        copy.wait()
        first = meta[2 + number]

        def place(block, carry, start=start, width=width, first=first):
            high, low = split(stage[start + block])
            where = first + (block // width) * slots + block % width
            panel[where, :, :order] = high
            panel[where, :, order:] = low
            return carry

        lax.fori_loop(0, rows * width, place, 0)
    left_base = meta[1]

    def load_left(block, carry):
        left[block, :order] = panel[left_base + block, :, :order]
        left[block, order:] = panel[left_base + block, :, order:]
        return carry

    lax.fori_loop(0, targets, load_left, 0)
    rounds = (meta[0] + UNROLL - 1) // UNROLL

    def product(result, factor):
        def step(turn, carry):
            sums = []
            for inner in range(UNROLL):
                begin = (turn * UNROLL + inner) * GROUP
                lhs = jnp.concatenate([left[left_list[begin + g]] for g in range(GROUP)], axis=1)
                rhs = jnp.concatenate([panel[right_list[begin + g]] for g in range(GROUP)], axis=0)
                both = jnp.dot(lhs, rhs, preferred_element_type=jnp.float32)
                sums.append(
                    both[:order, :order]
                    + (both[:order, order:] + both[order:, :order])
                    + both[order:, order:]
                )
            for inner in range(UNROLL):
                target = target_list[turn * UNROLL + inner]
                result[target] += sums[inner] if factor == 1.0 else factor * sums[inner]
            return carry

        lax.fori_loop(0, rounds, step, 0)

    product(square, 1.0)

    def middle(block, carry):
        value = square[block]
        high, low = split(value)
        left[block, :order] = high
        left[block, order:] = low
        out[block] = 3.0 * value
        return carry

    lax.fori_loop(0, targets, middle, 0)
    product(out, -2.0)


def products(total, left_base, firsts, lists, pieces, panel_rows, slots, rows):
    order = pieces[0].shape[-1]
    sizes = tuple((piece.shape[0], piece.shape[1]) for piece in pieces)
    targets = rows * slots
    meta = jnp.stack([jnp.asarray(v, jnp.int32) for v in (total, left_base, *firsts)])
    blocks = sum(a * b for a, b in sizes)
    any_spec = pl.BlockSpec(memory_space=pl.ANY)
    smem_spec = pl.BlockSpec(memory_space=pltpu.SMEM)
    return pl.pallas_call(
        functools.partial(kernel, sizes, slots, targets),
        out_shape=jax.ShapeDtypeStruct((targets, order, order), jnp.float32),
        in_specs=[smem_spec] * 4 + [any_spec] * len(pieces),
        out_specs=pl.BlockSpec(memory_space=pltpu.VMEM),
        scratch_shapes=[
            pltpu.VMEM((blocks, order, order), jnp.float32),
            pltpu.VMEM((panel_rows * slots, order, 2 * order), jnp.bfloat16),
            pltpu.VMEM((targets + 1, 2 * order, order), jnp.bfloat16),
            pltpu.VMEM((targets, order, order), jnp.float32),
            pltpu.SemaphoreType.DMA((len(pieces),)),
        ],
        compiler_params=pltpu.CompilerParams(vmem_limit_bytes=62 * 1024 * 1024),
        cost_estimate=pl.CostEstimate(
            flops=8 * targets * 8 * order**3,
            bytes_accessed=blocks * order * order * 4,
            transcendentals=0,
        ),
    )(meta, *lists, *[piece.reshape(-1, order, order) for piece in pieces])


def per_device(density, columns):
    local_rows, local_slots, order, _ = density.shape
    row_count = lax.axis_size("row")
    column_count = lax.axis_size("col")
    slots = local_slots * column_count
    rows = local_rows // column_count
    block_count = local_rows * row_count
    row_start = lax.axis_index("row") * local_rows
    column = lax.axis_index("col")
    own_start = column * rows
    if column_count == 2:
        numbers = range(2 * row_count)
        around = 2 * row_count

        def from_row(step):
            same = [(i, (i - 2 * step) % around) for i in numbers]
            cross = [(i, ((i ^ 1) - 2 * step) % around) for i in numbers]
            mine = lax.ppermute(columns, ("row", "col"), same) if step else columns
            peer = lax.ppermute(columns, ("row", "col"), cross)
            return mine, peer

        parts = [from_row(step) for step in (-1, 0, 1)]
        density, parts = lax.optimization_barrier((density, parts))
        before, full_columns, after = [
            jnp.where(
                column == 0,
                jnp.concatenate([mine, peer], axis=1),
                jnp.concatenate([peer, mine], axis=1),
            )
            for mine, peer in parts
        ]
    else:
        full_columns = lax.all_gather(columns, "col", axis=1, tiled=True)
        before = shifted(full_columns, 1)
        after = shifted(full_columns, -1)
    ext_columns = jnp.concatenate([before[local_rows - W :], full_columns, after[:W]])
    trimmed = column_count == 2 and local_rows == W
    panel_start = own_start if trimmed else 0
    total, *lists = work_lists(
        ext_columns, own_start, panel_start, row_start, block_count, rows
    )
    if trimmed:
        ring = [(2 * i, 2 * ((i + 1) % row_count)) for i in range(row_count)]
        back = [(2 * ((i + 1) % row_count) + 1, 2 * i + 1) for i in range(row_count)]
        far_pairs = ring + back
        near_pairs = [(b, a) for a, b in far_pairs]
        peers = [(i, i ^ 1) for i in range(2 * row_count)]
        axes = ("row", "col")
        near_at = column * rows
        rest_at = (1 - column) * rows
        own_near = lax.dynamic_slice_in_dim(density, near_at, rows)
        own_rest = lax.dynamic_slice_in_dim(density, rest_at, rows)
        other_near = lax.ppermute(own_rest, axes, peers)
        far_own = lax.ppermute(density, axes, far_pairs)
        near_own = lax.ppermute(own_near, axes, near_pairs)
        second, other_near = lax.optimization_barrier((own_near, other_near))
        other_rest = lax.ppermute(second, axes, peers)
        near_other = lax.ppermute(other_near, axes, near_pairs)
        far_other_near = lax.ppermute(other_near, axes, far_pairs)
        far_other_rest = lax.ppermute(other_rest, axes, far_pairs)
        pieces = [
            density,
            far_own,
            near_own,
            other_near,
            other_rest,
            near_other,
            far_other_near,
            far_other_rest,
        ]
        own_row = W - own_start
        far_row = jnp.where(column == 0, 0, rows + local_rows)
        near_row = jnp.where(column == 0, W + local_rows, 0)
        here = column * local_slots
        there = (1 - column) * local_slots
        firsts = [
            own_row * slots + here,
            far_row * slots + here,
            near_row * slots + here,
            (own_row + near_at) * slots + there,
            (own_row + rest_at) * slots + there,
            near_row * slots + there,
            (far_row + near_at) * slots + there,
            (far_row + rest_at) * slots + there,
        ]
        panel_rows = 2 * W + rows
    else:
        full_rows = lax.all_gather(density, "col", axis=1, tiled=True)
        pieces = [
            shifted(full_rows[local_rows - W :], 1),
            full_rows,
            shifted(full_rows[:W], -1),
        ]
        firsts = [0, W * slots, (W + local_rows) * slots]
        panel_rows = 2 * W + local_rows
    left_base = (W + own_start - panel_start) * slots
    result = products(total, left_base, firsts, lists, pieces, panel_rows, slots, rows)
    result = result.reshape(rows, slots, order, order)
    if column_count != 2:
        return lax.all_to_all(result, "col", split_axis=1, concat_axis=0, tiled=True)
    kept = lax.dynamic_slice_in_dim(result, column * local_slots, local_slots, axis=1)
    sent = lax.dynamic_slice_in_dim(result, (1 - column) * local_slots, local_slots, axis=1)
    arrived = lax.ppermute(sent, "col", [(0, 1), (1, 0)])
    return jnp.where(
        column == 0,
        jnp.concatenate([kept, arrived]),
        jnp.concatenate([arrived, kept]),
    )


def solution(mesh):
    in_specs = (P("row", "col", None, None), P("row", "col"))
    out_specs = P("row", "col", None, None)
    return jax.shard_map(
        per_device, mesh=mesh, in_specs=in_specs, out_specs=out_specs, check_vma=False
    )
```
